256 devices in a mesh: row: 16 (over z_hi, x), col: 16 (over y, z_lo, core).
Axes of the slice: x: 4, y: 4, z: 8 (z_hi: 4, z_lo: 2; z = z_hi * 2 + z_lo), core: 2. Of those that a mesh axis runs over, the one named last changes fastest.
Arguments:
- gradients: bfloat16 [256, 2, 524288], P(('row', 'col')), may hold values from -384 to 384
- master_params: float32 [2, 524288], P(None, ('row', 'col')), may hold values from -0.1 to 0.1
- first_moment: float32 [2, 524288], P(None, ('row', 'col')), may hold values from -3 to 3
- second_moment: float32 [2, 524288], P(None, ('row', 'col')), may hold values from 0.05 to 5
Outputs:
- new_master: float32 [2, 524288], P(None, ('row', 'col'))
- new_first: float32 [2, 524288], P(None, ('row', 'col'))
- new_second: float32 [2, 524288], P(None, ('row', 'col'))
- new_weights: bfloat16 [2, 524288], replicated
The draws below stay inside these ranges and needn't reach their ends.
All inputs are finite; a program needn't handle non-finite values.
Results may differ from the reference program's by a relative error of at most 0.009.
Values may be sent and summed in bfloat16 or wider, within the bound.
A program may use at most 64 MiB of HBM per device.

```python
import math
import jax
import jax.numpy as jnp
from jax import lax

LAYERS = 2
SLICE = 524288
DEVICES = 256


def spiked(result, rng, source, target, shards_of, factor):
    owner, partner = [(jnp.arange(result.shape[axis_at]) // (result.shape[axis_at] // shards_of)).reshape([-1 if axis == axis_at else 1 for axis in range(result.ndim)]) for axis_at in (source, target)]
    chosen = jax.random.permutation(rng, shards_of)[partner]
    strong = (owner == chosen) | (owner == (partner + shards_of // 2) % shards_of)
    return jnp.where(strong, factor * result, result)


def level_of(own_key, extent, split, smallest, largest):
    factor_of, own = 1.0, jax.random.fold_in(own_key, 6)
    for position, parts in split:
        heights = jnp.exp(jax.random.uniform(jax.random.fold_in(own, position), (parts,), jnp.float32, smallest / len(split), largest / len(split)))
        factor_of = factor_of * jnp.repeat(heights, extent[position] // parts).reshape([-1 if axis == position else 1 for axis in range(len(extent))])
    return factor_of


def gaussian(rng, dims, spread, most, split=(), held_as=jnp.bfloat16):
    result = jax.random.normal(rng, dims, jnp.float32) * spread
    if len(split) > 0:
        result = level_of(rng, dims, split, -0.22, 0.18) * result
    return jnp.clip(result, min=-most, max=most).astype(held_as)


def heavy_noise(own_key, dims, spread, bound, pieces, heavy, kind=jnp.bfloat16):
    drawn = spread * jax.random.normal(own_key, dims, jnp.float32)
    if pieces:
        drawn = drawn * level_of(own_key, dims, pieces, -0.22, 0.18)
    return jnp.clip(spiked(drawn, jax.random.fold_in(own_key, 3), *heavy), -bound, bound).astype(kind)


def setup_inputs(seed: int = 0) -> dict:
    splits = jax.random.split(jax.random.key(seed), 5)
    gradients = heavy_noise(splits[0], (DEVICES, LAYERS, SLICE), 16.0, 384.0, ((0, 256),), (0, 2, 256, 6.0))
    master_params = gaussian(splits[1], (LAYERS, SLICE), 0.025, 0.1, ((1, 256),), jnp.float32)
    first_moment = gaussian(splits[2], (LAYERS, SLICE), 0.5, 3.0, ((1, 256),), jnp.float32)
    second_moment = jnp.clip(jnp.exp(math.log(5.0) - 4.6051702 * jax.random.uniform(splits[3], (LAYERS, SLICE), jnp.float32) ** level_of(splits[3], (LAYERS, SLICE), ((1, 256),), -0.2, 0.2)), 0.05, 5.0)
    return {"gradients": gradients, "master_params": master_params, "first_moment": first_moment, "second_moment": second_moment}


beta_one = 0.9
beta_two = 0.95
learn_rate = 0.001
decay_rate = 0.1
epsilon = 1e-08
adam_step = 10.0

def adam_update(mean_grad, master_params, first_moment, second_moment):
    new_first = beta_one * first_moment + (1.0 - beta_one) * mean_grad
    new_second = beta_two * second_moment + (1.0 - beta_two) * mean_grad * mean_grad
    first_hat = new_first / (1.0 - beta_one ** adam_step)
    second_hat = new_second / (1.0 - beta_two ** adam_step)
    new_master = master_params - learn_rate * (first_hat / (jnp.sqrt(second_hat) + epsilon) + decay_rate * master_params)
    return (new_master, new_first, new_second)

def reference(gradients, master_params, first_moment, second_moment):
    mean_grad = lax.optimization_barrier(jnp.sum(gradients, axis=0, dtype=jnp.float32)) / DEVICES
    new_master, new_first, new_second = adam_update(mean_grad, master_params, first_moment, second_moment)
    return (new_master, new_first, new_second, new_master.astype(jnp.bfloat16))
```

```python
import jax
import jax.numpy as jnp
from jax import lax
from jax.experimental import pallas as pl
from jax.experimental.pallas import tpu as pltpu
from jax.sharding import PartitionSpec as P

beta_one = 0.9
beta_two = 0.95
learn_rate = 0.001
decay_rate = 0.1
epsilon = 1e-08
adam_step = 10.0

MESH = pl.DeviceIdType.MESH
F32 = jnp.float32
BF16 = jnp.bfloat16

PIECES = ((2, 0), (2, 1), (1, 1), (3, 0), (1, 0), (3, 1), (0, 0), (0, 1))


def adam_update(mean_grad, master_params, first_moment, second_moment):
    new_first = beta_one * first_moment + (1.0 - beta_one) * mean_grad
    new_second = beta_two * second_moment + (1.0 - beta_two) * mean_grad * mean_grad
    first_hat = new_first / (1.0 - beta_one**adam_step)
    second_hat = new_second / (1.0 - beta_two**adam_step)
    new_master = master_params - learn_rate * (
        first_hat / (jnp.sqrt(second_hat) + epsilon) + decay_rate * master_params
    )
    return (new_master, new_first, new_second)


def mod(value, size):
    return lax.rem(value, size)


def kernel(
    g, master, first, second,
    new_master, new_first, new_second, weights,
    own, given, sent1, got1, sum1, sent2, got2, sum2, got3, mine, theirs,
    load_sem, send0, recv0, send1, recv1, send2, recv2, send3, recv3,
    send4, recv4, send5, recv5, send6, recv6, send7, recv7, out_sem,
):
    row = lax.axis_index("row")
    col = lax.axis_index("col")
    z_hi = lax.div(row, 4)
    x = mod(row, 4)
    y = lax.div(col, 4)
    z_lo = mod(lax.div(col, 2), 2)
    core = mod(col, 2)
    z = z_hi * 2 + z_lo
    a = x + core * (y - x)
    b = y + core * (x - y)

    def device(a_of, b_of, z_of):
        x_of = a_of + core * (b_of - a_of)
        y_of = b_of + core * (a_of - b_of)
        return (lax.div(z_of, 2) * 4 + x_of, y_of * 4 + mod(z_of, 2) * 2 + core)

    partner = (row, col + 1 - 2 * core)
    a_right, a_left = device(mod(a + 1, 4), b, z), device(mod(a + 3, 4), b, z)
    b_right, b_left = device(a, mod(b + 1, 4), z), device(a, mod(b + 3, 4), z)
    along_z = [None] + [device(a, b, mod(z + k, 8)) for k in range(1, 8)]

    def remote(source, target, send_sem, recv_sem, where):
        return pltpu.make_async_remote_copy(
            src_ref=source, dst_ref=target, send_sem=send_sem, recv_sem=recv_sem,
            device_id=where, device_id_type=MESH,
        )

    barrier = pltpu.get_barrier_semaphore()
    peers = [partner, a_right, a_left, b_right, b_left] + along_z[1:]
    for peer in peers:
        pl.semaphore_signal(barrier, inc=1, device_id=peer, device_id_type=MESH)

    def part_of(core_v, place, half):
        zs = pl.ds(2 * half, 2)
        if core_v == 0:
            return (zs, place, slice(None), slice(None), 0)
        return (zs, slice(None), place, slice(None), 1)

    for core_v in (0, 1):
        @pl.when(core == core_v)
        def _():
            for k, (off, half) in enumerate(PIECES):
                source = g.at[part_of(core_v, mod(a + off, 4), half)]
                pltpu.make_async_copy(source, own.at[k], load_sem.at[k]).start()

    pl.semaphore_wait(barrier, len(peers))

    for core_v in (0, 1):
        @pl.when(core == core_v)
        def _():
            for k, (off, half) in enumerate(PIECES):
                source = g.at[part_of(1 - core_v, mod(b + off, 4), half)]
                remote(source, given.at[k], send0.at[k], recv0.at[k], partner).start()

    def piece_ready(k):
        pltpu.make_async_copy(own.at[k], own.at[k], load_sem.at[k]).wait()
        remote(own.at[k], given.at[k], send0.at[k], recv0.at[k], partner).wait_recv()

    def add_up(count, parts, store):
        def step(i, _):
            total = parts[0](i).astype(F32)
            for part in parts[1:]:
                total = total + part(i).astype(F32)
            store(i, total)
            return 0
        lax.fori_loop(0, count, step, 0)

    def block8(ref, k):
        return lambda i: ref[k, lax.div(i, 4), mod(i, 4)]

    def into_block8(ref, k):
        def store(i, value):
            ref[k, lax.div(i, 4), mod(i, 4)] = value.astype(BF16)
        return store

    to1 = (a_right, a_left, a_right, a_left, a_right, a_left)

    def ring1(k):
        return remote(sent1.at[k], got1.at[k], send1.at[k], recv1.at[k], to1[k])

    for k in range(4):
        piece_ready(k)
        add_up(8, [block8(own, k), block8(given, k)], into_block8(sent1, k))
        ring1(k).start()
    for k in (4, 5):
        piece_ready(k)
        ring1(k - 4).wait_recv()
        add_up(
            8, [block8(own, k), block8(given, k), block8(got1, k - 4)], into_block8(sent1, k)
        )
        ring1(k).start()
    piece_ready(6)
    piece_ready(7)

    def into_sum1(half):
        def store(i, value):
            sum1[mod(i, 4), 2 * half + lax.div(i, 4)] = value.astype(BF16)
        return store

    for half, (early, late) in enumerate(((3, 4), (2, 5))):
        ring1(early).wait_recv()
        ring1(late).wait_recv()
        add_up(
            8,
            [block8(own, 6 + half), block8(given, 6 + half), block8(got1, early), block8(got1, late)],
            into_sum1(half),
        )

    b_1, b_2, b_3 = mod(b + 1, 4), mod(b + 2, 4), mod(b + 3, 4)
    to2 = (b_right, b_left, b_right, b_left, b_right, b_left)

    def half2(place, half):
        return sum1.at[place, pl.ds(2 * half, 2)]

    from2 = (half2(b_2, 0), half2(b_2, 1), half2(b_1, 1), half2(b_3, 0), sent2.at[0], sent2.at[1])

    def ring2(k):
        return remote(from2[k], got2.at[k], send2.at[k], recv2.at[k], to2[k])

    for k in range(4):
        ring2(k).start()
    for k, (place, half) in ((4, (b_1, 0)), (5, (b_3, 1))):
        ring2(k - 4).wait_recv()
        def store(i, value):
            sent2[k - 4, i] = value.astype(BF16)
        add_up(
            2, [lambda i: sum1[place, 2 * half + i], lambda i: got2[k - 4, i]], store
        )
        ring2(k).start()
    for half, (early, late) in enumerate(((3, 4), (2, 5))):
        ring2(early).wait_recv()
        ring2(late).wait_recv()
        def store(i, value):
            sum2[2 * half + i] = value.astype(BF16)
        add_up(
            2,
            [lambda i: sum1[b, 2 * half + i], lambda i: got2[early, i], lambda i: got2[late, i]],
            store,
        )

    def across(k):
        z_of = mod(z + k, 8)
        return remote(
            sum2.at[lax.div(z_of, 2), mod(z_of, 2)], got3.at[k], send3.at[k], recv3.at[k], along_z[k]
        )

    order = (4, 3, 5, 2, 6, 1, 7)
    for k in order:
        across(k).start()
    total = sum2[z_hi, z_lo].astype(F32)
    for k in (1, 7, 2, 6, 3, 5, 4):
        across(k).wait_recv()
        total = total + got3[k].astype(F32)
    mean_grad = total / 256.0
    m_new, f_new, s_new = adam_update(mean_grad, master[...], first[...], second[...])
    new_master[...] = m_new
    new_first[...] = f_new
    new_second[...] = s_new
    mine[a, z_hi, b, z_lo] = m_new.astype(BF16)

    def gather_z(k):
        here = mine.at[a, z_hi, b, z_lo]
        return remote(here, here, send4.at[k], recv4.at[k], along_z[k])

    for k in order:
        gather_z(k).start()
    for k in (1, 7, 2, 6, 3, 5, 4):
        gather_z(k).wait_recv()

    def half5(place, half):
        return mine.at[a, pl.ds(2 * half, 2), place]

    send_what5 = ((b, 0), (b, 1), (b_3, 0), (b, 1), (b, 0), (b_1, 1))

    def gather_b(k):
        piece = half5(*send_what5[k])
        return remote(piece, piece, send5.at[k], recv5.at[k], b_right if k < 3 else b_left)

    for k in (0, 3, 1, 4):
        gather_b(k).start()
    gather_b(0).wait_recv()
    gather_b(2).start()
    gather_b(3).wait_recv()
    gather_b(5).start()
    for k in (1, 4, 2, 5):
        gather_b(k).wait_recv()

    a_1, a_2, a_3 = mod(a + 1, 4), mod(a + 2, 4), mod(a + 3, 4)

    def half6(ref, place, half):
        return ref.at[place, pl.ds(2 * half, 2)]

    send_what6 = ((a, 0), (a, 1), (a_3, 0), (a, 1), (a, 0), (a_1, 1))

    def gather_a(k):
        piece = half6(mine, *send_what6[k])
        return remote(piece, piece, send6.at[k], recv6.at[k], a_right if k < 3 else a_left)

    final = ((0, 0), (0, 1), (3, 0), (1, 1), (3, 1), (1, 0), (2, 0), (2, 1))

    def pass_on(j):
        off, half = final[j]
        place = mod(a + off, 4)
        return remote(
            half6(mine, place, half), half6(theirs, place, half), send7.at[j], recv7.at[j], partner
        )

    def write(j, from_partner):
        off, half = final[j]
        sem = out_sem.at[j + 8 * from_partner]
        for core_v in (0, 1):
            @pl.when(core == core_v)
            def _():
                if from_partner:
                    place = mod(b + off, 4)
                    pltpu.make_async_copy(
                        half6(theirs, place, half), weights.at[part_of(1 - core_v, place, half)], sem
                    ).start()
                else:
                    place = mod(a + off, 4)
                    pltpu.make_async_copy(
                        half6(mine, place, half), weights.at[part_of(core_v, place, half)], sem
                    ).start()

    for k in (0, 3, 1, 4):
        gather_a(k).start()
    pass_on(0).start()
    pass_on(1).start()
    write(0, 0)
    write(1, 0)
    for k, follow, j in ((0, 2, 2), (3, 5, 3), (1, None, 4), (4, None, 5), (2, None, 6), (5, None, 7)):
        gather_a(k).wait_recv()
        if follow is not None:
            gather_a(follow).start()
        pass_on(j).start()
        write(j, 0)
    for j in range(8):
        pass_on(j).wait_recv()
        write(j, 1)

    for k in range(8):
        remote(own.at[k], given.at[k], send0.at[k], recv0.at[k], partner).wait_send()
        pass_on(k).wait_send()
    for k in range(6):
        ring1(k).wait_send()
        ring2(k).wait_send()
        gather_b(k).wait_send()
        gather_a(k).wait_send()
    for k in range(1, 8):
        across(k).wait_send()
        gather_z(k).wait_send()
    for j in range(16):
        pltpu.make_async_copy(own.at[0], own.at[0], out_sem.at[j]).wait()


def as_rows(array):
    columns = array.shape[1]
    return array.reshape(2, columns // 128, 128).transpose(1, 0, 2).reshape(columns // 64, 128)


def from_rows(array):
    rows = array.shape[0]
    return array.reshape(rows // 2, 2, 128).transpose(1, 0, 2).reshape(2, rows * 64)


def shards(gradients, master_params, first_moment, second_moment):
    g = as_rows(gradients[0]).reshape(4, 4, 4, 2, 2, 32, 128)
    small = [as_rows(array) for array in (master_params, first_moment, second_moment)]
    dma = pltpu.SemaphoreType.DMA
    block = (2, 4, 2, 32, 128)
    vmem = pl.BlockSpec(memory_space=pltpu.VMEM)
    outs = pl.pallas_call(
        kernel,
        out_shape=[jax.ShapeDtypeStruct((32, 128), F32)] * 3
        + [jax.ShapeDtypeStruct(g.shape, BF16)],
        in_specs=[pl.BlockSpec(memory_space=pltpu.HBM)] + [vmem] * 3,
        out_specs=[vmem] * 3 + [pl.BlockSpec(memory_space=pltpu.HBM)],
        scratch_shapes=[
            pltpu.VMEM((8, *block), BF16),
            pltpu.VMEM((8, *block), BF16),
            pltpu.VMEM((6, *block), BF16),
            pltpu.VMEM((6, *block), BF16),
            pltpu.VMEM((4, 4, 2, 32, 128), BF16),
            pltpu.VMEM((2, 2, 2, 32, 128), BF16),
            pltpu.VMEM((6, 2, 2, 32, 128), BF16),
            pltpu.VMEM((4, 2, 32, 128), BF16),
            pltpu.VMEM((8, 32, 128), BF16),
            pltpu.VMEM((4, 4, 4, 2, 32, 128), BF16),
            pltpu.VMEM((4, 4, 4, 2, 32, 128), BF16),
            dma((8,)),
            dma((8,)), dma((8,)),
            dma((6,)), dma((6,)),
            dma((6,)), dma((6,)),
            dma((8,)), dma((8,)),
            dma((8,)), dma((8,)),
            dma((6,)), dma((6,)),
            dma((6,)), dma((6,)),
            dma((8,)), dma((8,)),
            dma((16,)),
        ],
        compiler_params=pltpu.CompilerParams(collective_id=0, has_side_effects=True),
        name="average_and_update",
    )(g, *small)
    new_master, new_first, new_second = [from_rows(array) for array in outs[:3]]
    return (new_master, new_first, new_second, from_rows(outs[3].reshape(8192, 128)))


def solution(mesh):
    in_specs = (
        P(("row", "col"), None, None),
        P(None, ("row", "col")),
        P(None, ("row", "col")),
        P(None, ("row", "col")),
    )
    out_specs = (P(None, ("row", "col")), P(None, ("row", "col")), P(None, ("row", "col")), P())
    return jax.shard_map(shards, mesh=mesh, in_specs=in_specs, out_specs=out_specs, check_vma=False)
```
